256 devices in a mesh: member: 8 (over y_lo, x), grid: 32 (over z, y_hi, core).
Axes of the slice: x: 4, y: 4 (y_hi: 2, y_lo: 2; y = y_hi * 2 + y_lo), z: 8, core: 2. Of those that a mesh axis runs over, the one named last changes fastest.
Arguments:
- prior_ensemble: bfloat16 [40, 48, 131072], P('member', None, 'grid'), may hold values from -6 to 6
- domain_site_mapping: int32 [32, 8, 512], P(None, None, 'grid'), may hold values from 0 to 4095, as said below
- neighbour_triples: int32 [32, 3, 4096], P('grid', None, 'member'), may hold values from 0 to 159
- stencil_factors: float32 [32, 3, 4096], P('grid', None, 'member'), may hold values from 0.1 to 1
- sparse_node_transforms: float32 [1600, 4096], P(None, 'grid'), may hold values from -0.4 to 1.8
Outputs:
- analysis: bfloat16 [40, 48, 131072], P('member', None, 'grid')
The draws below stay inside these ranges and needn't reach their ends.
Inputs may be any that keep to these rules, and one draw needn't show every extreme that they name: For every model patch h, the entries domain_site_mapping[:, :, h * 16 : (h + 1) * 16] hold every number from 0 to 4095 exactly once.
All inputs are finite; a program needn't handle non-finite values.
Results may differ from the reference program's by a relative error of at most 0.0076.
Values may be sent and summed in bfloat16 or wider, within the bound.
No kernel may reach another device: no remote copies, remote signals or barrier semaphores. Data moves between devices by JAX's collectives and lax.ppermute only.
A program may use at most 128 MiB of HBM per device.

```python
import math
import jax
import jax.numpy as jnp
from jax import lax

ENSEMBLE_SIZE = 40
STATE_QUANTITIES = 48
CELLS_DEV = 4096
COARSE_DEV = 128
RIM = 16
PATCHES = 32
GROUPS = 8
COLUMNS = 512
PER_SOURCE = 16
MESH_SITES = 131072
COARSE = 4096


def draw_domain_site_mapping(key, part):
    subkeys = jax.random.split(jax.random.fold_in(key, 11), PATCHES)
    shuffled = jax.vmap(lambda subkey: jax.random.permutation(subkey, CELLS_DEV))(subkeys)
    shuffled = shuffled.reshape(PATCHES, PATCHES, GROUPS, PER_SOURCE)
    return jnp.transpose(shuffled, (1, 2, 0, 3)).reshape(PATCHES, GROUPS, COLUMNS).astype(jnp.int32)


def draw_sparse_node_transforms(key, part):
    first_key = jax.random.fold_in(key, 21)
    second_key = jax.random.fold_in(key, 22)
    scatter_part = jnp.clip(0.12 * jax.random.normal(first_key, (ENSEMBLE_SIZE, ENSEMBLE_SIZE, COARSE), jnp.float32), -0.4, 0.4)
    diagonal_part = jax.random.uniform(second_key, (ENSEMBLE_SIZE, COARSE), jnp.float32, 0.6, 1.4)
    weights = scatter_part + jnp.eye(ENSEMBLE_SIZE, dtype=jnp.float32)[:, :, None] * diagonal_part[:, None, :]
    return weights.reshape(ENSEMBLE_SIZE * ENSEMBLE_SIZE, COARSE).astype(jnp.float32)


def place_ends(drawn, stream_key, smallest, high):
    spot = [jax.random.randint(jax.random.fold_in(stream_key, axis), (), 0, length) for axis, length in enumerate(drawn.shape)]
    widest = drawn.shape.index(max(drawn.shape))
    next_to = spot[:widest] + [(spot[widest] + 1) % drawn.shape[widest]] + spot[widest + 1:]
    return drawn.at[tuple(spot)].set(smallest).at[tuple(next_to)].set(high)


def shard_levels(rng, dims, cuts, low, top_value):
    factor_of = 1.0
    for dim, parts in cuts:
        steps = jax.random.uniform(jax.random.fold_in(jax.random.fold_in(rng, 6), dim), (parts,), jnp.float32, low / len(cuts), top_value / len(cuts))
        factor_of = factor_of * jnp.repeat(jnp.exp(steps), dims[dim] // parts).reshape((-1,) + (1,) * (len(dims) - 1 - dim))
    return factor_of


def scatter_about(stream_key, shape, scale, limit, pieces=(), kind=jnp.bfloat16):
    gain = shard_levels(stream_key, shape, pieces, -0.22, 0.18) if pieces else 1.0
    entries = jax.random.normal(stream_key, shape, jnp.float32) * scale * gain
    return jnp.minimum(jnp.maximum(entries, -limit), limit).astype(kind)


def setup_inputs(seed: int = 0) -> dict:
    seeds = jax.random.split(jax.random.key(seed), 6)
    return {
        "prior_ensemble": scatter_about(seeds[0], (ENSEMBLE_SIZE, STATE_QUANTITIES, MESH_SITES), 1.0, 6.0, ((0, 8), (2, 32))),
        "domain_site_mapping": draw_domain_site_mapping(jax.random.fold_in(seeds[5], 71), 0),
        "neighbour_triples": place_ends(jax.random.randint(seeds[2], (PATCHES, 3, CELLS_DEV), 0, COARSE_DEV + 2 * RIM), jax.random.fold_in(seeds[2], 1), 0, (COARSE_DEV + 2 * RIM) - 1).astype(jnp.int32),
        "stencil_factors": jnp.clip(jnp.exp(math.log(1.0) - 2.3025851 * jax.random.uniform(seeds[3], (PATCHES, 3, CELLS_DEV), jnp.float32) ** shard_levels(seeds[3], (PATCHES, 3, CELLS_DEV), ((0, 32), (2, 8)), -0.2, 0.2)), 0.1, 1.0),
        "sparse_node_transforms": draw_sparse_node_transforms(jax.random.fold_in(seeds[5], 71), 0),
    }


def reference(prior_ensemble, domain_site_mapping, neighbour_triples, stencil_factors, sparse_node_transforms):
    source_base = (jnp.arange(COLUMNS, dtype=jnp.int32) // PER_SOURCE) * CELLS_DEV
    cell_ids = (domain_site_mapping + source_base[None, None, :]).reshape(PATCHES, CELLS_DEV).astype(jnp.int32)

    def one_patch(inputs):
        sites_within_tile, points, raw_share, patch_id = inputs
        arriving_analysis_slots = jnp.take(prior_ensemble, sites_within_tile, axis=2)
        member_mean = jnp.sum(arriving_analysis_slots, axis=0, dtype=jnp.float32) / ENSEMBLE_SIZE
        deviation = (arriving_analysis_slots.astype(jnp.float32) - member_mean[None]).astype(jnp.bfloat16)
        coarse_ids = ((patch_id * COARSE_DEV - RIM + points) % COARSE).astype(jnp.int32)
        shares = raw_share / jnp.sum(raw_share, axis=0, keepdims=True)
        blended = jnp.zeros((ENSEMBLE_SIZE * ENSEMBLE_SIZE, CELLS_DEV), jnp.float32)
        for which in range(3):
            blended = blended + jnp.take(sparse_node_transforms, coarse_ids[which], axis=1) * shares[which][None, :]
        blended = blended.reshape(ENSEMBLE_SIZE, ENSEMBLE_SIZE, CELLS_DEV).astype(jnp.bfloat16)
        result = jnp.einsum('kfc,kjc->jfc', deviation.astype(jnp.float32), blended.astype(jnp.float32)) + member_mean[None]
        return result.astype(jnp.bfloat16)

    patch_list = jnp.arange(PATCHES, dtype=jnp.int32)
    results = lax.map(one_patch, (cell_ids, neighbour_triples, stencil_factors, patch_list))
    ordered = jnp.moveaxis(results, 0, 2).reshape(ENSEMBLE_SIZE, STATE_QUANTITIES, MESH_SITES)
    analysis = jnp.zeros((ENSEMBLE_SIZE, STATE_QUANTITIES, MESH_SITES), jnp.bfloat16)
    analysis = analysis.at[:, :, cell_ids.reshape(-1)].set(ordered)
    return analysis
```

```python
import jax
import jax.numpy as jnp
from jax import lax
from jax.experimental import pallas as pl
from jax.experimental.pallas import tpu as pltpu
from jax.sharding import PartitionSpec as P

ENSEMBLE_SIZE = 40
RIM = 16
VMEM_LIMIT = 48 * 1024 * 1024


def full_spec(shape):
    return pl.BlockSpec(shape, lambda *_: (0,) * len(shape))


def pick_kernel(rows_ref, targets_ref, out_ref):
    cells = rows_ref.shape[1]
    columns = targets_ref.shape[2]
    cell_ids = lax.broadcasted_iota(jnp.int32, (cells, columns), 0)
    onehot = jnp.where(cell_ids == targets_ref[0], 1.0, 0.0).astype(jnp.bfloat16)
    out_ref[0] = jnp.dot(rows_ref[...], onehot, preferred_element_type=jnp.float32).astype(
        jnp.bfloat16
    )


def pick_columns(source_rows, targets):
    rows, cells = source_rows.shape
    groups, _, columns = targets.shape
    return pl.pallas_call(
        pick_kernel,
        grid=(groups,),
        in_specs=[
            full_spec((rows, cells)),
            pl.BlockSpec((1, 1, columns), lambda i: (i, 0, 0)),
        ],
        out_specs=pl.BlockSpec((1, rows, columns), lambda i: (i, 0, 0)),
        out_shape=jax.ShapeDtypeStruct((groups, rows, columns), jnp.bfloat16),
        compiler_params=pltpu.CompilerParams(vmem_limit_bytes=VMEM_LIMIT),
        name="pick",
    )(source_rows, targets)


def place_kernel(parts_ref, positions_ref, out_ref, rows_ref):
    groups, _, columns = parts_ref.shape
    block = out_ref.shape[1]
    step = pl.program_id(0)

    @pl.when(step == 0)
    def _():
        for group in range(groups):
            rows_ref[:, group * columns : (group + 1) * columns] = parts_ref[group]

    positions = positions_ref[...]
    lanes = positions.shape[1]
    wide = jnp.concatenate([positions] * (block // lanes), axis=1)
    target_ids = step * block + lax.broadcasted_iota(jnp.int32, (groups * columns, block), 1)
    onehot = jnp.where(wide == target_ids, 1.0, 0.0).astype(jnp.bfloat16)
    out_ref[...] = jnp.dot(
        rows_ref[...], onehot, preferred_element_type=jnp.float32
    ).astype(jnp.bfloat16)


def place_columns(parts, positions):
    groups, rows, columns = parts.shape
    cells = groups * columns
    return pl.pallas_call(
        place_kernel,
        grid=(groups,),
        in_specs=[full_spec(parts.shape), full_spec(positions.shape)],
        out_specs=pl.BlockSpec((rows, columns), lambda i: (0, i)),
        out_shape=jax.ShapeDtypeStruct((rows, cells), jnp.bfloat16),
        scratch_shapes=[pltpu.VMEM((rows, cells), jnp.bfloat16)],
        compiler_params=pltpu.CompilerParams(vmem_limit_bytes=VMEM_LIMIT),
        name="place",
    )(parts, positions)


def turn_kernel(transforms_ref, out_ref):
    out_ref[...] = jnp.transpose(transforms_ref[...]).astype(jnp.bfloat16)


def turn(transforms):
    entries, points = transforms.shape
    return pl.pallas_call(
        turn_kernel,
        out_shape=jax.ShapeDtypeStruct((points, entries), jnp.bfloat16),
        compiler_params=pltpu.CompilerParams(vmem_limit_bytes=VMEM_LIMIT),
        name="turn",
    )(transforms)


def blend_kernel(left_ref, own_ref, right_ref, points_ref, factors_ref, out_ref):
    rim, points_own = left_ref.shape[0], own_ref.shape[0]
    columns = points_ref.shape[2]
    extent = points_own + 2 * rim
    factors = factors_ref[0]
    shares = factors / jnp.sum(factors, axis=0, keepdims=True)
    slot_ids = lax.broadcasted_iota(jnp.int32, (extent, columns), 0)
    spread = jnp.zeros((extent, columns), jnp.float32)
    for which in range(3):
        spread = spread + jnp.where(
            points_ref[0, which : which + 1, :] == slot_ids, shares[which : which + 1, :], 0.0
        )
    high = spread.astype(jnp.bfloat16)
    low = (spread - high.astype(jnp.float32)).astype(jnp.bfloat16)
    widened = jnp.concatenate([left_ref[...], own_ref[...], right_ref[...]], axis=0)
    dims = (((0,), (0,)), ((), ()))
    out_ref[...] = lax.dot_general(
        jnp.concatenate([high, low], axis=0),
        jnp.concatenate([widened, widened], axis=0),
        dims,
        preferred_element_type=jnp.float32,
    ).astype(jnp.bfloat16)


def blend(left, own, right, points, factors):
    return pl.pallas_call(
        blend_kernel,
        out_shape=jax.ShapeDtypeStruct((points.shape[2], own.shape[1]), jnp.bfloat16),
        compiler_params=pltpu.CompilerParams(vmem_limit_bytes=VMEM_LIMIT),
        name="blend",
    )(left, own, right, points, factors)


def update_kernel(fields_ref, weights_ref, out_ref, turned_ref, deviation_ref, mean_ref):
    members, fields, lanes = fields_ref.shape
    turned_ref[...] = jnp.transpose(weights_ref[...].astype(jnp.float32))
    total = fields_ref[0].astype(jnp.float32)
    for k in range(1, members):
        total = total + fields_ref[k].astype(jnp.float32)
    mean = total * (1.0 / members)
    mean_ref[...] = mean
    for k in range(members):
        deviation = (fields_ref[k].astype(jnp.float32) - mean).astype(jnp.bfloat16)
        deviation_ref[k] = deviation.astype(jnp.float32)
    together = 4

    def body(step, carry):
        base = step * together
        sums = [mean_ref[...] for _ in range(together)]
        for k in range(members):
            deviation = deviation_ref[k]
            for t in range(together):
                weight = turned_ref[pl.ds(k * members + base + t, 1), :]
                sums[t] = sums[t] + deviation * weight
        for t in range(together):
            out_ref[base + t] = sums[t].astype(jnp.bfloat16)
        return carry

    lax.fori_loop(0, members // together, body, 0)


def update(fields, weights):
    members, quantities, columns = fields.shape
    lanes = 128
    return pl.pallas_call(
        update_kernel,
        grid=(columns // lanes,),
        in_specs=[
            pl.BlockSpec((members, quantities, lanes), lambda i: (0, 0, i)),
            pl.BlockSpec((lanes, members * members), lambda i: (i, 0)),
        ],
        out_specs=pl.BlockSpec((members, quantities, lanes), lambda i: (0, 0, i)),
        out_shape=jax.ShapeDtypeStruct(fields.shape, jnp.bfloat16),
        scratch_shapes=[
            pltpu.VMEM((members * members, lanes), jnp.float32),
            pltpu.VMEM((members, quantities, lanes), jnp.float32),
            pltpu.VMEM((quantities, lanes), jnp.float32),
        ],
        compiler_params=pltpu.CompilerParams(vmem_limit_bytes=VMEM_LIMIT),
        name="update",
    )(fields, weights)


def on_device(
    prior_ensemble, domain_site_mapping, neighbour_triples, stencil_factors, sparse_node_transforms
):
    own_members, quantities, cells = prior_ensemble.shape
    groups = lax.axis_size("member")
    patches = lax.axis_size("grid")
    columns = cells // groups
    per_source = columns // patches
    entries = ENSEMBLE_SIZE * ENSEMBLE_SIZE

    turned = turn(sparse_node_transforms)
    following = [(i, (i + 1) % patches) for i in range(patches)]
    preceding = [((i + 1) % patches, i) for i in range(patches)]
    left = lax.ppermute(turned[-RIM:], "grid", following)
    right = lax.ppermute(turned[:RIM], "grid", preceding)

    order = jnp.transpose(domain_site_mapping, (1, 0, 2)).reshape(groups, 1, columns)
    source_rows = prior_ensemble.reshape(own_members * quantities, cells)
    chosen = pick_columns(source_rows, order)
    blended = blend(left, turned, right, neighbour_triples, stencil_factors)
    weights = lax.all_to_all(
        blended.reshape(patches, per_source, entries), "grid", split_axis=0, concat_axis=0, tiled=True
    ).reshape(columns, entries)
    gathered = lax.all_to_all(chosen, "member", split_axis=0, concat_axis=0, tiled=True)
    result = update(gathered.reshape(ENSEMBLE_SIZE, quantities, columns), weights)
    returned = lax.all_to_all(
        result.reshape(groups, own_members * quantities, columns),
        "member",
        split_axis=0,
        concat_axis=0,
        tiled=True,
    )
    positions = jnp.broadcast_to(order.reshape(cells, 1), (cells, 128))
    placed = place_columns(returned, positions)
    return placed.reshape(own_members, quantities, cells)


def solution(mesh):
    return jax.shard_map(
        on_device,
        mesh=mesh,
        in_specs=(
            P("member", None, "grid"),
            P(None, None, "grid"),
            P("grid", None, "member"),
            P("grid", None, "member"),
            P(None, "grid"),
        ),
        out_specs=P("member", None, "grid"),
        check_vma=False,
    )
```

```python
import functools

import jax
import jax.numpy as jnp
from jax import lax
from jax.experimental import pallas as pl
from jax.experimental.pallas import tpu as pltpu
from jax.sharding import PartitionSpec as P


ENSEMBLE_SIZE = 40
RIM = 16
LANES = 128
MIB = 1024 * 1024
STEPS = [2, 6, 7, 5, 3, 1, 4, 0]
TOGETHER = 2
PLACED = 4


def cost(flops, moved):
    return pl.CostEstimate(flops=int(flops), bytes_accessed=int(moved), transcendentals=0)


def full_spec(shape):
    return pl.BlockSpec(shape, lambda *_: (0,) * len(shape))


def pick_kernel(rows_ref, targets_ref, out_ref):
    cells = rows_ref.shape[1]
    columns = targets_ref.shape[1]
    cell_ids = lax.broadcasted_iota(jnp.int32, (cells, columns), 0)
    onehot = jnp.where(cell_ids == targets_ref[...], 1.0, 0.0).astype(jnp.bfloat16)
    out_ref[...] = jnp.dot(
        rows_ref[...], onehot, preferred_element_type=jnp.float32
    ).astype(jnp.bfloat16)


def pick_columns(source_rows, targets):
    rows, cells = source_rows.shape
    columns = targets.shape[1]
    return pl.pallas_call(
        pick_kernel,
        out_shape=jax.ShapeDtypeStruct((rows, columns), jnp.bfloat16),
        compiler_params=pltpu.CompilerParams(vmem_limit_bytes=24 * MIB),
        cost_estimate=cost(2 * rows * cells * columns, 2 * rows * columns),
        name="pick",
    )(source_rows, targets)


def place_kernel(*refs, count, more):
    part_refs, positions_ref = refs[:count], refs[count]
    out_ref = refs[-1]
    block = out_ref.shape[1]
    parts = jnp.concatenate([ref[...] for ref in part_refs], axis=1)
    wide = jnp.concatenate([positions_ref[...]] * (block // LANES), axis=1)
    first = pl.program_id(0) * block
    target_ids = first + lax.broadcasted_iota(jnp.int32, wide.shape, 1)
    onehot = jnp.where(wide == target_ids, 1.0, 0.0).astype(jnp.bfloat16)
    placed = jnp.dot(parts, onehot, preferred_element_type=jnp.float32)
    if more:
        placed = placed + refs[count + 1][...].astype(jnp.float32)
    out_ref[...] = placed.astype(jnp.bfloat16)


def place_columns(parts, positions, before, cells):
    rows, columns = parts[0].shape
    block = 512
    more = before is not None
    block_spec = pl.BlockSpec((rows, block), lambda i: (0, i))
    operands = [*parts, positions]
    specs = [full_spec(operand.shape) for operand in operands]
    if more:
        operands.append(before)
        specs.append(block_spec)
    return pl.pallas_call(
        functools.partial(place_kernel, count=len(parts), more=more),
        grid=(cells // block,),
        in_specs=specs,
        out_specs=block_spec,
        out_shape=jax.ShapeDtypeStruct((rows, cells), jnp.bfloat16),
        compiler_params=pltpu.CompilerParams(vmem_limit_bytes=32 * MIB),
        cost_estimate=cost(2 * rows * cells * columns * len(parts), 4 * rows * cells),
        name="place",
    )(*operands)


def turn_kernel(transforms_ref, out_ref):
    out_ref[...] = jnp.transpose(transforms_ref[...]).astype(jnp.bfloat16)


def turn(transforms):
    entries, points = transforms.shape
    return pl.pallas_call(
        turn_kernel,
        out_shape=jax.ShapeDtypeStruct((points, entries), jnp.bfloat16),
        compiler_params=pltpu.CompilerParams(vmem_limit_bytes=24 * MIB),
        cost_estimate=cost(1e8, 6 * entries * points),
        name="turn",
    )(transforms)


def blend_kernel(left_ref, own_ref, right_ref, points_ref, factors_ref, out_ref):
    rim, points_own = left_ref.shape[0], own_ref.shape[0]
    columns = points_ref.shape[2]
    extent = points_own + 2 * rim
    factors = [factors_ref[which] for which in range(3)]
    total = factors[0] + factors[1] + factors[2]
    shares = [factor / total for factor in factors]
    slot_ids = lax.broadcasted_iota(jnp.int32, (extent, columns), 0)
    spread = jnp.zeros((extent, columns), jnp.float32)
    for which in range(3):
        spread = spread + jnp.where(
            points_ref[which] == slot_ids, shares[which], 0.0
        )
    high = spread.astype(jnp.bfloat16)
    low = (spread - high.astype(jnp.float32)).astype(jnp.bfloat16)
    widened = jnp.concatenate([left_ref[...], own_ref[...], right_ref[...]], axis=0)
    dims = (((0,), (0,)), ((), ()))
    out_ref[...] = lax.dot_general(
        jnp.concatenate([high, low], axis=0),
        jnp.concatenate([widened, widened], axis=0),
        dims,
        preferred_element_type=jnp.float32,
    ).astype(jnp.bfloat16)


def blend(left, own, right, points, factors):
    return pl.pallas_call(
        blend_kernel,
        out_shape=jax.ShapeDtypeStruct((points.shape[2], own.shape[1]), jnp.bfloat16),
        compiler_params=pltpu.CompilerParams(vmem_limit_bytes=24 * MIB),
        cost_estimate=cost(1e9, 4e6),
        name="blend",
    )(left, own, right, points, factors)


def center_kernel(*refs):
    *field_refs, deviation_ref, mean_ref = refs
    own = field_refs[0].shape[0]
    total = jnp.zeros(mean_ref.shape, jnp.float32)
    for ref in field_refs:
        for k in range(own):
            total = total + ref[k].astype(jnp.float32)
    mean = total * (1.0 / ENSEMBLE_SIZE)
    mean_ref[...] = mean
    for s, ref in enumerate(field_refs):
        for k in range(own):
            deviation_ref[s * own + k] = (ref[k].astype(jnp.float32) - mean).astype(jnp.bfloat16)


def center(fields):
    own, quantities, columns = fields[0].shape
    block = lambda i: (0, 0, i)
    return pl.pallas_call(
        center_kernel,
        grid=(columns // LANES,),
        in_specs=[pl.BlockSpec((own, quantities, LANES), block)] * len(fields),
        out_specs=[
            pl.BlockSpec((ENSEMBLE_SIZE, quantities, LANES), block),
            pl.BlockSpec((quantities, LANES), lambda i: (0, i)),
        ],
        out_shape=[
            jax.ShapeDtypeStruct((ENSEMBLE_SIZE, quantities, columns), jnp.bfloat16),
            jax.ShapeDtypeStruct((quantities, columns), jnp.float32),
        ],
        compiler_params=pltpu.CompilerParams(vmem_limit_bytes=24 * MIB),
        cost_estimate=cost(1e9, 4e6),
        name="center",
    )(*fields)


def tip_kernel(weights_ref, out_ref):
    out_ref[0] = jnp.transpose(weights_ref[...].astype(jnp.float32))


def tip(weights):
    columns, entries = weights.shape
    return pl.pallas_call(
        tip_kernel,
        grid=(columns // LANES,),
        in_specs=[pl.BlockSpec((LANES, entries), lambda i: (i, 0))],
        out_specs=pl.BlockSpec((1, entries, LANES), lambda i: (i, 0, 0)),
        out_shape=jax.ShapeDtypeStruct((columns // LANES, entries, LANES), jnp.float32),
        compiler_params=pltpu.CompilerParams(vmem_limit_bytes=24 * MIB),
        cost_estimate=cost(1e9, 4e6),
        name="tip",
    )(weights)


def update_kernel(group_ref, weights_ref, deviation_ref, mean_ref, *out_refs, steps):
    own = out_refs[0].shape[0]
    groups = ENSEMBLE_SIZE // own
    for step, out_ref in zip(steps, out_refs):
        first = group_ref[step] * own
        sums = [mean_ref[...] for _ in range(own)]
        for s in range(groups):
            start = group_ref[s] * (own * ENSEMBLE_SIZE) + first
            for k in range(own):
                deviation = deviation_ref[s * own + k].astype(jnp.float32)
                for j in range(own):
                    weight = weights_ref[0, pl.ds(start + k * ENSEMBLE_SIZE + j, 1), :]
                    sums[j] = sums[j] + deviation * weight
        for j in range(own):
            out_ref[j] = sums[j].astype(jnp.bfloat16)


def update(group, steps, weights, deviation, mean):
    members, quantities, columns = deviation.shape
    own = ENSEMBLE_SIZE // group.shape[0]
    block = lambda i, *_: (0, 0, i)
    return pl.pallas_call(
        functools.partial(update_kernel, steps=tuple(steps)),
        grid_spec=pltpu.PrefetchScalarGridSpec(
            num_scalar_prefetch=1,
            grid=(columns // LANES,),
            in_specs=[
                pl.BlockSpec((1, weights.shape[1], LANES), lambda i, *_: (i, 0, 0)),
                pl.BlockSpec((members, quantities, LANES), block),
                pl.BlockSpec((quantities, LANES), lambda i, *_: (0, i)),
            ],
            out_specs=[pl.BlockSpec((own, quantities, LANES), block)] * len(steps),
        ),
        out_shape=[jax.ShapeDtypeStruct((own, quantities, columns), jnp.bfloat16)] * len(steps),
        compiler_params=pltpu.CompilerParams(vmem_limit_bytes=24 * MIB),
        cost_estimate=cost(3e9 * len(steps), 8e6),
        name="update",
    )(group, weights, deviation, mean)


def exchange(part, s, groups):
    if s == 0:
        return part
    return lax.ppermute(part, "member", [(i, i ^ s) for i in range(groups)])


def local_step(
    prior_ensemble, domain_site_mapping, neighbour_triples, stencil_factors, sparse_node_transforms
):
    own_members, quantities, cells = prior_ensemble.shape
    groups = lax.axis_size("member")
    patches = lax.axis_size("grid")
    columns = cells // groups
    per_source = columns // patches
    entries = ENSEMBLE_SIZE * ENSEMBLE_SIZE
    rows = own_members * quantities

    turned = turn(sparse_node_transforms)
    following = [(i, (i + 1) % patches) for i in range(patches)]
    preceding = [((i + 1) % patches, i) for i in range(patches)]
    left = lax.ppermute(turned[-RIM:], "grid", following)
    right = lax.ppermute(turned[:RIM], "grid", preceding)
    blended = blend(
        left,
        turned,
        right,
        jnp.transpose(neighbour_triples, (1, 0, 2)),
        jnp.transpose(stencil_factors, (1, 0, 2)),
    )
    weights = lax.all_to_all(
        blended.reshape(patches, per_source, entries),
        "grid",
        split_axis=0,
        concat_axis=0,
        tiled=True,
    ).reshape(columns, entries)

    group = (lax.axis_index("member") ^ jnp.arange(groups, dtype=jnp.int32)).astype(jnp.int32)
    order = jnp.transpose(domain_site_mapping, (1, 0, 2)).reshape(groups, columns)[group]
    source_rows = prior_ensemble.reshape(rows, cells)
    steps = STEPS
    fields = [None] * groups
    for s in steps:
        chosen = pick_columns(source_rows, order[s : s + 1])
        fields[s] = exchange(chosen, s, groups).reshape(own_members, quantities, columns)
    deviation, mean = center(fields)
    spread = tip(weights)
    positions = jnp.broadcast_to(order[jnp.array(steps)].reshape(cells, 1), (cells, LANES))
    results = []
    for first in range(0, groups, TOGETHER):
        now = steps[first : first + TOGETHER]
        parts = update(group, now, spread, deviation, mean)
        for s, part in zip(now, parts):
            results.append(exchange(part.reshape(rows, columns), s, groups))
    placed = None
    for first in range(0, groups, PLACED):
        placed = place_columns(
            results[first : first + PLACED],
            positions[first * columns : (first + PLACED) * columns],
            placed,
            cells,
        )
    return placed.reshape(own_members, quantities, cells)


def solution(mesh):
    return jax.shard_map(
        local_step,
        mesh=mesh,
        in_specs=(
            P("member", None, "grid"),
            P(None, None, "grid"),
            P("grid", None, "member"),
            P("grid", None, "member"),
            P(None, "grid"),
        ),
        out_specs=P("member", None, "grid"),
        check_vma=False,
    )
```

```python
import functools

import jax
import jax.numpy as jnp
from jax import lax
from jax.experimental import pallas as pl
from jax.experimental.pallas import tpu as pltpu
from jax.sharding import PartitionSpec as P


ENSEMBLE_SIZE = 40
RIM = 16
LANES = 128
MIB = 1024 * 1024
STEPS = [6, 7, 5, 4, 2, 3, 1, 0]
TOGETHER = 2


def cost(flops, moved):
    return pl.CostEstimate(flops=int(flops), bytes_accessed=int(moved), transcendentals=0)


def pick_kernel(rows_ref, targets_ref, out_ref):
    cells = rows_ref.shape[1]
    columns = targets_ref.shape[1]
    cell_ids = lax.broadcasted_iota(jnp.int32, (cells, columns), 0)
    onehot = jnp.where(cell_ids == targets_ref[...], 1.0, 0.0).astype(jnp.bfloat16)
    out_ref[...] = jnp.dot(
        rows_ref[...], onehot, preferred_element_type=jnp.float32
    ).astype(jnp.bfloat16)


def pick_columns(source_rows, targets):
    rows, cells = source_rows.shape
    columns = targets.shape[1]
    return pl.pallas_call(
        pick_kernel,
        out_shape=jax.ShapeDtypeStruct((rows, columns), jnp.bfloat16),
        compiler_params=pltpu.CompilerParams(vmem_limit_bytes=24 * MIB),
        cost_estimate=cost(2 * rows * cells * columns, 2 * rows * columns),
        name="pick",
    )(source_rows, targets)


def place_kernel(*refs):
    *part_refs, positions_ref, out_ref, rows_ref = refs
    columns = part_refs[0].shape[1]
    block = out_ref.shape[1]
    step = pl.program_id(0)

    @pl.when(step == 0)
    def _():
        for at, ref in enumerate(part_refs):
            rows_ref[:, at * columns : (at + 1) * columns] = ref[...]

    wide = jnp.concatenate([positions_ref[...]] * (block // LANES), axis=1)
    target_ids = step * block + lax.broadcasted_iota(jnp.int32, wide.shape, 1)
    onehot = jnp.where(wide == target_ids, 1.0, 0.0).astype(jnp.bfloat16)
    out_ref[...] = jnp.dot(
        rows_ref[...], onehot, preferred_element_type=jnp.float32
    ).astype(jnp.bfloat16)


def place_columns(parts, positions):
    rows, columns = parts[0].shape
    cells = columns * len(parts)
    block = 512
    whole = pl.BlockSpec(memory_space=pltpu.VMEM)
    return pl.pallas_call(
        place_kernel,
        grid=(cells // block,),
        in_specs=[whole] * (len(parts) + 1),
        out_specs=pl.BlockSpec((rows, block), lambda i: (0, i)),
        out_shape=jax.ShapeDtypeStruct((rows, cells), jnp.bfloat16),
        scratch_shapes=[pltpu.VMEM((rows, cells), jnp.bfloat16)],
        compiler_params=pltpu.CompilerParams(vmem_limit_bytes=24 * MIB),
        cost_estimate=cost(2 * rows * cells * cells, 4 * rows * cells),
        name="place",
    )(*parts, positions)


def turn_kernel(transforms_ref, out_ref):
    out_ref[...] = jnp.transpose(transforms_ref[...]).astype(jnp.bfloat16)


def turn(transforms):
    entries, points = transforms.shape
    return pl.pallas_call(
        turn_kernel,
        out_shape=jax.ShapeDtypeStruct((points, entries), jnp.bfloat16),
        compiler_params=pltpu.CompilerParams(vmem_limit_bytes=24 * MIB),
        cost_estimate=cost(1e8, 6 * entries * points),
        name="turn",
    )(transforms)


def weigh_kernel(points_ref, factors_ref, out_ref):
    extent, columns = out_ref.shape[0] // 2, out_ref.shape[1]
    factors = [factors_ref[which] for which in range(3)]
    total = factors[0] + factors[1] + factors[2]
    slot_ids = lax.broadcasted_iota(jnp.int32, (extent, columns), 0)
    spread = jnp.zeros((extent, columns), jnp.float32)
    for which in range(3):
        spread = spread + jnp.where(points_ref[which] == slot_ids, factors[which] / total, 0.0)
    high = spread.astype(jnp.bfloat16)
    out_ref[:extent] = high
    out_ref[extent:] = (spread - high.astype(jnp.float32)).astype(jnp.bfloat16)


def weigh(points, factors, extent):
    return pl.pallas_call(
        weigh_kernel,
        out_shape=jax.ShapeDtypeStruct((2 * extent, points.shape[2]), jnp.bfloat16),
        compiler_params=pltpu.CompilerParams(vmem_limit_bytes=16 * MIB),
        cost_estimate=cost(1e8, 4e5),
        name="weigh",
    )(points, factors)


def blend_kernel(left_ref, own_ref, right_ref, pieces_ref, out_ref):
    widened = jnp.concatenate([left_ref[...], own_ref[...], right_ref[...]], axis=0)
    out_ref[...] = lax.dot_general(
        pieces_ref[...],
        jnp.concatenate([widened, widened], axis=0),
        (((0,), (0,)), ((), ())),
        preferred_element_type=jnp.float32,
    ).astype(jnp.bfloat16)


def blend(left, own, right, pieces):
    return pl.pallas_call(
        blend_kernel,
        out_shape=jax.ShapeDtypeStruct((pieces.shape[1], own.shape[1]), jnp.bfloat16),
        compiler_params=pltpu.CompilerParams(vmem_limit_bytes=16 * MIB),
        cost_estimate=cost(1e9, 4e6),
        name="blend",
    )(left, own, right, pieces)


def center_kernel(*refs):
    *field_refs, deviation_ref, mean_ref = refs
    own = field_refs[0].shape[0]
    total = jnp.zeros(mean_ref.shape[1:], jnp.float32)
    for ref in field_refs:
        for k in range(own):
            total = total + ref[k].astype(jnp.float32)
    mean = total * (1.0 / ENSEMBLE_SIZE)
    mean_ref[0] = mean
    for s, ref in enumerate(field_refs):
        for k in range(own):
            deviation_ref[0, s * own + k] = (ref[k].astype(jnp.float32) - mean).astype(jnp.bfloat16)


def center(fields):
    own, quantities, columns = fields[0].shape
    blocks = columns // LANES
    block = lambda i: (0, 0, i)
    return pl.pallas_call(
        center_kernel,
        grid=(columns // LANES,),
        in_specs=[pl.BlockSpec((own, quantities, LANES), block)] * len(fields),
        out_specs=[
            pl.BlockSpec((1, ENSEMBLE_SIZE, quantities, LANES), lambda i: (i, 0, 0, 0)),
            pl.BlockSpec((1, quantities, LANES), lambda i: (i, 0, 0)),
        ],
        out_shape=[
            jax.ShapeDtypeStruct((blocks, ENSEMBLE_SIZE, quantities, LANES), jnp.bfloat16),
            jax.ShapeDtypeStruct((blocks, quantities, LANES), jnp.float32),
        ],
        compiler_params=pltpu.CompilerParams(vmem_limit_bytes=24 * MIB),
        cost_estimate=cost(1e9, 4e6),
        name="center",
    )(*fields)


def tip_kernel(weights_ref, out_ref):
    out_ref[0] = jnp.transpose(weights_ref[...].astype(jnp.float32))


def tip(weights):
    columns, entries = weights.shape
    return pl.pallas_call(
        tip_kernel,
        grid=(columns // LANES,),
        in_specs=[pl.BlockSpec((LANES, entries), lambda i: (i, 0))],
        out_specs=pl.BlockSpec((1, entries, LANES), lambda i: (i, 0, 0)),
        out_shape=jax.ShapeDtypeStruct((columns // LANES, entries, LANES), jnp.float32),
        compiler_params=pltpu.CompilerParams(vmem_limit_bytes=24 * MIB),
        cost_estimate=cost(1e9, 4e6),
        name="tip",
    )(weights)


def update_kernel(group_ref, weights_ref, deviation_ref, mean_ref, *out_refs, steps):
    own = out_refs[0].shape[0]
    groups = ENSEMBLE_SIZE // own
    for step, out_ref in zip(steps, out_refs):
        first = group_ref[step] * own
        for block in range(weights_ref.shape[0]):

            def body(pair, sums):
                sums = list(sums)
                for half in range(2):
                    s = 2 * pair + half
                    start = group_ref[s] * (own * ENSEMBLE_SIZE) + first
                    for k in range(own):
                        deviation = deviation_ref[block, s * own + k].astype(jnp.float32)
                        for j in range(own):
                            row = pl.ds(start + k * ENSEMBLE_SIZE + j, 1)
                            sums[j] = sums[j] + deviation * weights_ref[block, row, :]
                return tuple(sums)

            sums = lax.fori_loop(
                0, groups // 2, body, tuple(mean_ref[block] for _ in range(own))
            )
            for j in range(own):
                out_ref[j, :, block * LANES : (block + 1) * LANES] = sums[j].astype(jnp.bfloat16)


def update(group, steps, weights, deviation, mean):
    blocks, _, quantities, lanes = deviation.shape
    own = ENSEMBLE_SIZE // group.shape[0]
    whole = pl.BlockSpec(memory_space=pltpu.VMEM)
    return pl.pallas_call(
        functools.partial(update_kernel, steps=tuple(steps)),
        in_specs=[pl.BlockSpec(memory_space=pltpu.SMEM), whole, whole, whole],
        out_specs=[whole] * len(steps),
        out_shape=[jax.ShapeDtypeStruct((own, quantities, blocks * lanes), jnp.bfloat16)]
        * len(steps),
        compiler_params=pltpu.CompilerParams(vmem_limit_bytes=16 * MIB),
        cost_estimate=cost(3e9 * len(steps), 8e6),
        name="update",
    )(group, weights, deviation, mean)


def exchange(part, s, groups):
    if s == 0:
        return part
    return lax.ppermute(part, "member", [(i, i ^ s) for i in range(groups)])


def local_step(
    prior_ensemble, domain_site_mapping, neighbour_triples, stencil_factors, sparse_node_transforms
):
    own_members, quantities, cells = prior_ensemble.shape
    groups = lax.axis_size("member")
    patches = lax.axis_size("grid")
    columns = cells // groups
    per_source = columns // patches
    entries = ENSEMBLE_SIZE * ENSEMBLE_SIZE
    rows = own_members * quantities

    turned = turn(sparse_node_transforms)
    following = [(i, (i + 1) % patches) for i in range(patches)]
    preceding = [((i + 1) % patches, i) for i in range(patches)]
    left = lax.ppermute(turned[-RIM:], "grid", following)
    right = lax.ppermute(turned[:RIM], "grid", preceding)
    pieces = weigh(
        jnp.transpose(neighbour_triples, (1, 0, 2)),
        jnp.transpose(stencil_factors, (1, 0, 2)),
        turned.shape[0] + 2 * RIM,
    )
    blended = blend(left, turned, right, pieces)
    weights = lax.all_to_all(
        blended.reshape(patches, per_source, entries),
        "grid",
        split_axis=0,
        concat_axis=0,
        tiled=True,
    ).reshape(columns, entries)

    group = (lax.axis_index("member") ^ jnp.arange(groups, dtype=jnp.int32)).astype(jnp.int32)
    order = jnp.transpose(domain_site_mapping, (1, 0, 2)).reshape(groups, columns)[group]
    source_rows = prior_ensemble.reshape(rows, cells)
    steps = STEPS
    fields = [None] * groups
    for s in steps:
        chosen = pick_columns(source_rows, order[s : s + 1])
        fields[s] = exchange(chosen, s, groups).reshape(own_members, quantities, columns)
    deviation, mean = center(fields)
    spread = tip(weights)
    results = {}
    for first in range(0, groups, TOGETHER):
        now = steps[first : first + TOGETHER]
        parts = update(group, now, spread, deviation, mean)
        for s, part in zip(now, parts):
            results[s] = exchange(part.reshape(rows, columns), s, groups)
    positions = jnp.broadcast_to(order.reshape(cells, 1), (cells, LANES))
    placed = place_columns([results[s] for s in range(groups)], positions)
    return placed.reshape(own_members, quantities, cells)


def solution(mesh):
    return jax.shard_map(
        local_step,
        mesh=mesh,
        in_specs=(
            P("member", None, "grid"),
            P(None, None, "grid"),
            P("grid", None, "member"),
            P("grid", None, "member"),
            P(None, "grid"),
        ),
        out_specs=P("member", None, "grid"),
        check_vma=False,
    )
```

```python
import functools

import jax
import jax.numpy as jnp
from jax import lax
from jax.experimental import pallas as pl
from jax.experimental.pallas import tpu as pltpu
from jax.sharding import PartitionSpec as P


ENSEMBLE_SIZE = 40
RIM = 16
LANES = 128
MIB = 1024 * 1024
STEPS = [6, 7, 5, 4, 2, 3, 1, 0]
TOGETHER = 2
PLACED = [[6, 7, 0], [5, 4, 2, 3, 1]]


def cost(flops, moved):
    return pl.CostEstimate(flops=int(flops), bytes_accessed=int(moved), transcendentals=0)


def pick_kernel(rows_ref, targets_ref, out_ref):
    cells = rows_ref.shape[1]
    cell_ids = lax.broadcasted_iota(jnp.int32, (cells, targets_ref.shape[2]), 0)
    onehot = jnp.where(cell_ids == targets_ref[0], 1.0, 0.0).astype(jnp.bfloat16)
    out_ref[0] = jnp.dot(
        rows_ref[...], onehot, preferred_element_type=jnp.float32
    ).astype(jnp.bfloat16)


def pick_columns(source_rows, targets):
    rows, cells = source_rows.shape
    count, _, columns = targets.shape
    return pl.pallas_call(
        pick_kernel,
        grid=(count,),
        in_specs=[
            pl.BlockSpec(memory_space=pltpu.VMEM),
            pl.BlockSpec((1, 1, columns), lambda i: (i, 0, 0)),
        ],
        out_specs=pl.BlockSpec((1, rows, columns), lambda i: (i, 0, 0)),
        out_shape=jax.ShapeDtypeStruct((count, rows, columns), jnp.bfloat16),
        compiler_params=pltpu.CompilerParams(vmem_limit_bytes=24 * MIB),
        cost_estimate=cost(2 * count * rows * cells * columns, 2 * count * rows * columns),
        name="pick",
    )(source_rows, targets)


def place_kernel(*refs, count, more):
    part_refs, positions_ref = refs[:count], refs[count]
    out_ref, rows_ref = refs[-2:]
    columns = part_refs[0].shape[1]
    block = out_ref.shape[1]
    step = pl.program_id(0)

    @pl.when(step == 0)
    def _():
        for at, ref in enumerate(part_refs):
            rows_ref[:, at * columns : (at + 1) * columns] = ref[...]

    wide = jnp.concatenate([positions_ref[...]] * (block // LANES), axis=1)
    target_ids = step * block + lax.broadcasted_iota(jnp.int32, wide.shape, 1)
    onehot = jnp.where(wide == target_ids, 1.0, 0.0).astype(jnp.bfloat16)
    placed = jnp.dot(rows_ref[...], onehot, preferred_element_type=jnp.float32)
    if more:
        placed = placed + refs[count + 1][...].astype(jnp.float32)
    out_ref[...] = placed.astype(jnp.bfloat16)


def place_columns(parts, positions, before, cells):
    rows, columns = parts[0].shape
    block = 512
    whole = pl.BlockSpec(memory_space=pltpu.VMEM)
    block_spec = pl.BlockSpec((rows, block), lambda i: (0, i))
    more = before is not None
    return pl.pallas_call(
        functools.partial(place_kernel, count=len(parts), more=more),
        grid=(cells // block,),
        in_specs=[whole] * (len(parts) + 1) + [block_spec] * more,
        out_specs=block_spec,
        out_shape=jax.ShapeDtypeStruct((rows, cells), jnp.bfloat16),
        scratch_shapes=[pltpu.VMEM((rows, columns * len(parts)), jnp.bfloat16)],
        compiler_params=pltpu.CompilerParams(vmem_limit_bytes=20 * MIB),
        cost_estimate=cost(2 * rows * cells * columns * len(parts), 4 * rows * cells),
        name="place",
    )(*parts, positions, *([before] if more else []))


def turn_kernel(transforms_ref, out_ref):
    out_ref[...] = jnp.transpose(transforms_ref[...]).astype(jnp.bfloat16)


def turn(transforms):
    entries, points = transforms.shape
    return pl.pallas_call(
        turn_kernel,
        out_shape=jax.ShapeDtypeStruct((points, entries), jnp.bfloat16),
        compiler_params=pltpu.CompilerParams(vmem_limit_bytes=24 * MIB),
        cost_estimate=cost(1e8, 6 * entries * points),
        name="turn",
    )(transforms)


def weigh_kernel(points_ref, factors_ref, out_ref):
    extent, columns = out_ref.shape[0] // 2, out_ref.shape[1]
    factors = [factors_ref[which] for which in range(3)]
    total = factors[0] + factors[1] + factors[2]
    slot_ids = lax.broadcasted_iota(jnp.int32, (extent, columns), 0)
    spread = jnp.zeros((extent, columns), jnp.float32)
    for which in range(3):
        spread = spread + jnp.where(points_ref[which] == slot_ids, factors[which] / total, 0.0)
    high = spread.astype(jnp.bfloat16)
    out_ref[:extent] = high
    out_ref[extent:] = (spread - high.astype(jnp.float32)).astype(jnp.bfloat16)


def weigh(points, factors, extent):
    return pl.pallas_call(
        weigh_kernel,
        out_shape=jax.ShapeDtypeStruct((2 * extent, points.shape[2]), jnp.bfloat16),
        compiler_params=pltpu.CompilerParams(vmem_limit_bytes=16 * MIB),
        cost_estimate=cost(1e8, 4e5),
        name="weigh",
    )(points, factors)


def blend_kernel(left_ref, own_ref, right_ref, pieces_ref, out_ref):
    widened = jnp.concatenate([left_ref[...], own_ref[...], right_ref[...]], axis=0)
    out_ref[...] = lax.dot_general(
        pieces_ref[...],
        jnp.concatenate([widened, widened], axis=0),
        (((0,), (0,)), ((), ())),
        preferred_element_type=jnp.float32,
    ).astype(jnp.bfloat16)


def blend(left, own, right, pieces):
    return pl.pallas_call(
        blend_kernel,
        out_shape=jax.ShapeDtypeStruct((pieces.shape[1], own.shape[1]), jnp.bfloat16),
        compiler_params=pltpu.CompilerParams(vmem_limit_bytes=16 * MIB),
        cost_estimate=cost(1e9, 4e6),
        name="blend",
    )(left, own, right, pieces)


def center_kernel(*refs):
    *field_refs, deviation_ref, mean_ref = refs
    own = field_refs[0].shape[0]
    total = jnp.zeros(mean_ref.shape[1:], jnp.float32)
    for ref in field_refs:
        for k in range(own):
            total = total + ref[k].astype(jnp.float32)
    mean = total * (1.0 / ENSEMBLE_SIZE)
    mean_ref[0] = mean
    for s, ref in enumerate(field_refs):
        for k in range(own):
            deviation_ref[0, s * own + k] = (ref[k].astype(jnp.float32) - mean).astype(jnp.bfloat16)


def center(fields):
    own, quantities, columns = fields[0].shape
    blocks = columns // LANES
    block = lambda i: (0, 0, i)
    return pl.pallas_call(
        center_kernel,
        grid=(columns // LANES,),
        in_specs=[pl.BlockSpec((own, quantities, LANES), block)] * len(fields),
        out_specs=[
            pl.BlockSpec((1, ENSEMBLE_SIZE, quantities, LANES), lambda i: (i, 0, 0, 0)),
            pl.BlockSpec((1, quantities, LANES), lambda i: (i, 0, 0)),
        ],
        out_shape=[
            jax.ShapeDtypeStruct((blocks, ENSEMBLE_SIZE, quantities, LANES), jnp.bfloat16),
            jax.ShapeDtypeStruct((blocks, quantities, LANES), jnp.float32),
        ],
        compiler_params=pltpu.CompilerParams(vmem_limit_bytes=24 * MIB),
        cost_estimate=cost(1e9, 4e6),
        name="center",
    )(*fields)


def tip_kernel(weights_ref, out_ref):
    out_ref[0] = jnp.transpose(weights_ref[...].astype(jnp.float32))


def tip(weights):
    columns, entries = weights.shape
    return pl.pallas_call(
        tip_kernel,
        grid=(columns // LANES,),
        in_specs=[pl.BlockSpec((LANES, entries), lambda i: (i, 0))],
        out_specs=pl.BlockSpec((1, entries, LANES), lambda i: (i, 0, 0)),
        out_shape=jax.ShapeDtypeStruct((columns // LANES, entries, LANES), jnp.float32),
        compiler_params=pltpu.CompilerParams(vmem_limit_bytes=24 * MIB),
        cost_estimate=cost(1e9, 4e6),
        name="tip",
    )(weights)


def update_kernel(group_ref, weights_ref, deviation_ref, mean_ref, *out_refs, steps):
    own = out_refs[0].shape[0]
    groups = ENSEMBLE_SIZE // own
    for step, out_ref in zip(steps, out_refs):
        first = group_ref[step] * own
        for block in range(weights_ref.shape[0]):

            def body(pair, sums):
                sums = list(sums)
                for half in range(2):
                    s = 2 * pair + half
                    start = group_ref[s] * (own * ENSEMBLE_SIZE) + first
                    for k in range(own):
                        deviation = deviation_ref[block, s * own + k].astype(jnp.float32)
                        for j in range(own):
                            row = pl.ds(start + k * ENSEMBLE_SIZE + j, 1)
                            sums[j] = sums[j] + deviation * weights_ref[block, row, :]
                return tuple(sums)

            sums = lax.fori_loop(
                0, groups // 2, body, tuple(mean_ref[block] for _ in range(own))
            )
            for j in range(own):
                out_ref[j, :, block * LANES : (block + 1) * LANES] = sums[j].astype(jnp.bfloat16)


def update(group, steps, weights, deviation, mean):
    blocks, _, quantities, lanes = deviation.shape
    own = ENSEMBLE_SIZE // group.shape[0]
    whole = pl.BlockSpec(memory_space=pltpu.VMEM)
    return pl.pallas_call(
        functools.partial(update_kernel, steps=tuple(steps)),
        in_specs=[pl.BlockSpec(memory_space=pltpu.SMEM), whole, whole, whole],
        out_specs=[whole] * len(steps),
        out_shape=[jax.ShapeDtypeStruct((own, quantities, blocks * lanes), jnp.bfloat16)]
        * len(steps),
        compiler_params=pltpu.CompilerParams(vmem_limit_bytes=16 * MIB),
        cost_estimate=cost(3e9 * len(steps), 8e6),
        name="update",
    )(group, weights, deviation, mean)


def exchange(part, s, groups):
    if s == 0:
        return part
    return lax.ppermute(part, "member", [(i, i ^ s) for i in range(groups)])


def local_step(
    prior_ensemble, domain_site_mapping, neighbour_triples, stencil_factors, sparse_node_transforms
):
    own_members, quantities, cells = prior_ensemble.shape
    groups = lax.axis_size("member")
    patches = lax.axis_size("grid")
    columns = cells // groups
    per_source = columns // patches
    entries = ENSEMBLE_SIZE * ENSEMBLE_SIZE
    rows = own_members * quantities

    turned = turn(sparse_node_transforms)
    following = [(i, (i + 1) % patches) for i in range(patches)]
    preceding = [((i + 1) % patches, i) for i in range(patches)]
    left = lax.ppermute(turned[-RIM:], "grid", following)
    right = lax.ppermute(turned[:RIM], "grid", preceding)
    pieces = weigh(
        jnp.transpose(neighbour_triples, (1, 0, 2)),
        jnp.transpose(stencil_factors, (1, 0, 2)),
        turned.shape[0] + 2 * RIM,
    )
    blended = blend(left, turned, right, pieces)
    weights = lax.all_to_all(
        blended.reshape(patches, per_source, entries),
        "grid",
        split_axis=0,
        concat_axis=0,
        tiled=True,
    ).reshape(columns, entries)

    group = (lax.axis_index("member") ^ jnp.arange(groups, dtype=jnp.int32)).astype(jnp.int32)
    order = jnp.transpose(domain_site_mapping, (1, 0, 2)).reshape(groups, columns)[group]
    source_rows = prior_ensemble.reshape(rows, cells)
    steps = STEPS
    half = groups // 2
    targets = order.reshape(groups, 1, columns)
    crossing = pick_columns(source_rows, targets[half:])
    arrived = exchange(crossing, half, groups)
    fields = [None] * groups
    fields[half] = arrived[0]
    for s in range(1, half):
        chosen = pick_columns(source_rows, targets[s : s + 1])
        fields[s] = exchange(chosen[0], s, groups)
    fields[0] = pick_columns(source_rows, targets[:1])[0]
    for s in range(1, half):
        fields[half + s] = exchange(arrived[s], s, groups)
    fields = [part.reshape(own_members, quantities, columns) for part in fields]
    deviation, mean = center(fields)
    spread = tip(weights)
    results = {}
    for first in range(0, groups, TOGETHER):
        now = steps[first : first + TOGETHER]
        parts = update(group, now, spread, deviation, mean)
        for s, part in zip(now, parts):
            results[s] = exchange(part.reshape(rows, columns), s, groups)
    placed = None
    for now in PLACED:
        positions = jnp.concatenate([order[s] for s in now]).reshape(-1, 1)
        positions = jnp.broadcast_to(positions, (positions.shape[0], LANES))
        placed = place_columns([results[s] for s in now], positions, placed, cells)
    return placed.reshape(own_members, quantities, cells)


def solution(mesh):
    return jax.shard_map(
        local_step,
        mesh=mesh,
        in_specs=(
            P("member", None, "grid"),
            P(None, None, "grid"),
            P("grid", None, "member"),
            P("grid", None, "member"),
            P(None, "grid"),
        ),
        out_specs=P("member", None, "grid"),
        check_vma=False,
    )
```

```python
import functools

import jax
import jax.numpy as jnp
from jax import lax
from jax.experimental import pallas as pl
from jax.experimental.pallas import tpu as pltpu
from jax.sharding import PartitionSpec as P


ENSEMBLE_SIZE = 40
RIM = 16
LANES = 128
MIB = 1024 * 1024
STEPS = [6, 7, 5, 4, 2, 3, 1, 0]
TOGETHER = 2
BLEND = 256
PLACED = [[6, 7, 5, 0], [4, 2, 3, 1]]


def cost(flops, moved):
    return pl.CostEstimate(flops=int(flops), bytes_accessed=int(moved), transcendentals=0)


def pick_kernel(rows_ref, targets_ref, out_ref):
    cells = rows_ref.shape[1]
    cell_ids = lax.broadcasted_iota(jnp.int32, (cells, targets_ref.shape[2]), 0)
    onehot = jnp.where(cell_ids == targets_ref[0], 1.0, 0.0).astype(jnp.bfloat16)
    out_ref[0] = jnp.dot(
        rows_ref[...], onehot, preferred_element_type=jnp.float32
    ).astype(jnp.bfloat16)


def pick_columns(source_rows, targets):
    rows, cells = source_rows.shape
    count, _, columns = targets.shape
    return pl.pallas_call(
        pick_kernel,
        grid=(count,),
        in_specs=[
            pl.BlockSpec(memory_space=pltpu.VMEM),
            pl.BlockSpec((1, 1, columns), lambda i: (i, 0, 0)),
        ],
        out_specs=pl.BlockSpec((1, rows, columns), lambda i: (i, 0, 0)),
        out_shape=jax.ShapeDtypeStruct((count, rows, columns), jnp.bfloat16),
        compiler_params=pltpu.CompilerParams(vmem_limit_bytes=24 * MIB),
        cost_estimate=cost(2 * count * rows * cells * columns, 2 * count * rows * columns),
        name="pick",
    )(source_rows, targets)


def place_kernel(*refs, count, more):
    part_refs, positions_ref = refs[:count], refs[count]
    out_ref, rows_ref = refs[-2:]
    columns = part_refs[0].shape[1]
    block = out_ref.shape[1]
    step = pl.program_id(0)

    @pl.when(step == 0)
    def _():
        for at, ref in enumerate(part_refs):
            rows_ref[:, at * columns : (at + 1) * columns] = ref[...]

    wide = jnp.concatenate([positions_ref[...]] * (block // LANES), axis=1)
    target_ids = step * block + lax.broadcasted_iota(jnp.int32, wide.shape, 1)
    onehot = jnp.where(wide == target_ids, 1.0, 0.0).astype(jnp.bfloat16)
    placed = jnp.dot(rows_ref[...], onehot, preferred_element_type=jnp.float32)
    if more:
        placed = placed + refs[count + 1][...].astype(jnp.float32)
    out_ref[...] = placed.astype(jnp.bfloat16)


def place_columns(parts, positions, before, cells):
    rows, columns = parts[0].shape
    block = 1024
    whole = pl.BlockSpec(memory_space=pltpu.VMEM)
    block_spec = pl.BlockSpec((rows, block), lambda i: (0, i))
    more = before is not None
    return pl.pallas_call(
        functools.partial(place_kernel, count=len(parts), more=more),
        grid=(cells // block,),
        in_specs=[whole] * (len(parts) + 1) + [block_spec] * more,
        out_specs=block_spec,
        out_shape=jax.ShapeDtypeStruct((rows, cells), jnp.bfloat16),
        scratch_shapes=[pltpu.VMEM((rows, columns * len(parts)), jnp.bfloat16)],
        compiler_params=pltpu.CompilerParams(vmem_limit_bytes=32 * MIB),
        cost_estimate=cost(2 * rows * cells * columns * len(parts), 4 * rows * cells),
        name="place",
    )(*parts, positions, *([before] if more else []))


def turn_kernel(transforms_ref, *refs):
    head_ref, out_ref, tail_ref = refs[-3:]
    turned = jnp.transpose(transforms_ref[...]).astype(jnp.bfloat16)
    head_ref[...] = turned[:RIM]
    out_ref[...] = turned
    tail_ref[...] = turned[-RIM:]


def turn(transforms, *before):
    entries, points = transforms.shape
    return pl.pallas_call(
        turn_kernel,
        out_shape=[
            jax.ShapeDtypeStruct((count, entries), jnp.bfloat16) for count in (RIM, points, RIM)
        ],
        compiler_params=pltpu.CompilerParams(vmem_limit_bytes=12 * MIB),
        cost_estimate=cost(2e9, 6 * entries * points),
        name="turn",
    )(transforms, *before)


def weigh_kernel(points_ref, factors_ref, out_ref):
    extent, columns = out_ref.shape[0] // 2, out_ref.shape[1]
    factors = [factors_ref[which] for which in range(3)]
    total = factors[0] + factors[1] + factors[2]
    slot_ids = lax.broadcasted_iota(jnp.int32, (extent, columns), 0)
    spread = jnp.zeros((extent, columns), jnp.float32)
    for which in range(3):
        spread = spread + jnp.where(points_ref[which] == slot_ids, factors[which] / total, 0.0)
    high = spread.astype(jnp.bfloat16)
    out_ref[:extent] = high
    out_ref[extent:] = (spread - high.astype(jnp.float32)).astype(jnp.bfloat16)


def weigh(points, factors, extent):
    return pl.pallas_call(
        weigh_kernel,
        out_shape=jax.ShapeDtypeStruct((2 * extent, points.shape[2]), jnp.bfloat16),
        compiler_params=pltpu.CompilerParams(vmem_limit_bytes=16 * MIB),
        cost_estimate=cost(1e8, 4e5),
        name="weigh",
    )(points, factors)


def blend_kernel(left_ref, own_ref, right_ref, pieces_ref, out_ref):
    widened = jnp.concatenate([left_ref[...], own_ref[...], right_ref[...]], axis=0)
    out_ref[...] = lax.dot_general(
        pieces_ref[...],
        jnp.concatenate([widened, widened], axis=0),
        (((0,), (0,)), ((), ())),
        preferred_element_type=jnp.float32,
    ).astype(jnp.bfloat16)


def blend(left, own, right, pieces):
    columns, entries = pieces.shape[1], own.shape[1]
    block = BLEND
    whole = pl.BlockSpec(memory_space=pltpu.VMEM)
    return pl.pallas_call(
        blend_kernel,
        grid=(columns // block,),
        in_specs=[whole, whole, whole, pl.BlockSpec((pieces.shape[0], block), lambda i: (0, i))],
        out_specs=pl.BlockSpec((block, entries), lambda i: (i, 0)),
        out_shape=jax.ShapeDtypeStruct((columns, entries), jnp.bfloat16),
        compiler_params=pltpu.CompilerParams(vmem_limit_bytes=16 * MIB),
        cost_estimate=cost(1e9, 4e6),
        name="blend",
    )(left, own, right, pieces)


def center_kernel(*refs):
    *field_refs, deviation_ref, mean_ref = refs
    own = field_refs[0].shape[0]
    total = jnp.zeros(mean_ref.shape[1:], jnp.float32)
    for ref in field_refs:
        for k in range(own):
            total = total + ref[k].astype(jnp.float32)
    mean = total * (1.0 / ENSEMBLE_SIZE)
    mean_ref[0] = mean
    for s, ref in enumerate(field_refs):
        for k in range(own):
            deviation_ref[0, s * own + k] = (ref[k].astype(jnp.float32) - mean).astype(jnp.bfloat16)


def center(fields):
    own, quantities, columns = fields[0].shape
    blocks = columns // LANES
    block = lambda i: (0, 0, i)
    return pl.pallas_call(
        center_kernel,
        grid=(columns // LANES,),
        in_specs=[pl.BlockSpec((own, quantities, LANES), block)] * len(fields),
        out_specs=[
            pl.BlockSpec((1, ENSEMBLE_SIZE, quantities, LANES), lambda i: (i, 0, 0, 0)),
            pl.BlockSpec((1, quantities, LANES), lambda i: (i, 0, 0)),
        ],
        out_shape=[
            jax.ShapeDtypeStruct((blocks, ENSEMBLE_SIZE, quantities, LANES), jnp.bfloat16),
            jax.ShapeDtypeStruct((blocks, quantities, LANES), jnp.float32),
        ],
        compiler_params=pltpu.CompilerParams(vmem_limit_bytes=24 * MIB),
        cost_estimate=cost(1e9, 4e6),
        name="center",
    )(*fields)


def tip_kernel(weights_ref, out_ref):
    out_ref[0] = jnp.transpose(weights_ref[...].astype(jnp.float32))


def tip(weights):
    columns, entries = weights.shape
    return pl.pallas_call(
        tip_kernel,
        grid=(columns // LANES,),
        in_specs=[pl.BlockSpec((LANES, entries), lambda i: (i, 0))],
        out_specs=pl.BlockSpec((1, entries, LANES), lambda i: (i, 0, 0)),
        out_shape=jax.ShapeDtypeStruct((columns // LANES, entries, LANES), jnp.float32),
        compiler_params=pltpu.CompilerParams(vmem_limit_bytes=24 * MIB),
        cost_estimate=cost(1e9, 4e6),
        name="tip",
    )(weights)


def update_kernel(group_ref, weights_ref, deviation_ref, mean_ref, *out_refs, steps):
    own = out_refs[0].shape[0]
    groups = ENSEMBLE_SIZE // own
    for step, out_ref in zip(steps, out_refs):
        first = group_ref[step] * own
        for block in range(weights_ref.shape[0]):

            def body(pair, sums):
                sums = list(sums)
                for half in range(2):
                    s = 2 * pair + half
                    start = group_ref[s] * (own * ENSEMBLE_SIZE) + first
                    for k in range(own):
                        deviation = deviation_ref[block, s * own + k].astype(jnp.float32)
                        for j in range(own):
                            row = pl.ds(start + k * ENSEMBLE_SIZE + j, 1)
                            sums[j] = sums[j] + deviation * weights_ref[block, row, :]
                return tuple(sums)

            sums = lax.fori_loop(
                0, groups // 2, body, tuple(mean_ref[block] for _ in range(own))
            )
            for j in range(own):
                out_ref[j, :, block * LANES : (block + 1) * LANES] = sums[j].astype(jnp.bfloat16)


def update(group, steps, weights, deviation, mean):
    blocks, _, quantities, lanes = deviation.shape
    own = ENSEMBLE_SIZE // group.shape[0]
    whole = pl.BlockSpec(memory_space=pltpu.VMEM)
    return pl.pallas_call(
        functools.partial(update_kernel, steps=tuple(steps)),
        in_specs=[pl.BlockSpec(memory_space=pltpu.SMEM), whole, whole, whole],
        out_specs=[whole] * len(steps),
        out_shape=[jax.ShapeDtypeStruct((own, quantities, blocks * lanes), jnp.bfloat16)]
        * len(steps),
        compiler_params=pltpu.CompilerParams(vmem_limit_bytes=16 * MIB),
        cost_estimate=cost(3e9 * len(steps), 8e6),
        name="update",
    )(group, weights, deviation, mean)


def exchange(part, s, groups):
    if s == 0:
        return part
    return lax.ppermute(part, "member", [(i, i ^ s) for i in range(groups)])


def local_step(
    prior_ensemble, domain_site_mapping, neighbour_triples, stencil_factors, sparse_node_transforms
):
    own_members, quantities, cells = prior_ensemble.shape
    groups = lax.axis_size("member")
    patches = lax.axis_size("grid")
    columns = cells // groups
    per_source = columns // patches
    entries = ENSEMBLE_SIZE * ENSEMBLE_SIZE
    rows = own_members * quantities

    targets = jnp.transpose(domain_site_mapping, (1, 0, 2)).reshape(groups, 1, columns)
    source_rows = prior_ensemble.reshape(rows, cells)
    head, turned, tail = turn(sparse_node_transforms)
    following = [(i, (i + 1) % patches) for i in range(patches)]
    preceding = [((i + 1) % patches, i) for i in range(patches)]
    left = lax.ppermute(tail, "grid", following)
    right = lax.ppermute(head, "grid", preceding)
    pieces = weigh(
        jnp.transpose(neighbour_triples, (1, 0, 2)),
        jnp.transpose(stencil_factors, (1, 0, 2)),
        turned.shape[0] + 2 * RIM,
    )
    blended = blend(left, turned, right, pieces)
    weights = lax.all_to_all(
        blended.reshape(patches, per_source, entries),
        "grid",
        split_axis=0,
        concat_axis=0,
        tiled=True,
    ).reshape(columns, entries)

    group = (lax.axis_index("member") ^ jnp.arange(groups, dtype=jnp.int32)).astype(jnp.int32)
    order = targets.reshape(groups, columns)[group]
    later = order.reshape(groups, 1, columns)
    steps = STEPS
    half = groups // 2
    crossing = pick_columns(source_rows, later[half + 2 :])
    arrived = exchange(crossing, half, groups)
    crossing = pick_columns(source_rows, later[half : half + 2])
    more = exchange(crossing, half, groups)
    arrived = [more[0], more[1], arrived[0], arrived[1]]
    fields = [None] * groups
    fields[half] = arrived[0]
    for s in range(1, half):
        chosen = pick_columns(source_rows, later[s : s + 1])
        fields[s] = exchange(chosen[0], s, groups)
    fields[0] = pick_columns(source_rows, later[:1])[0]
    for s in range(1, half):
        fields[half + s] = exchange(arrived[s], s, groups)
    fields = [part.reshape(own_members, quantities, columns) for part in fields]
    deviation, mean = center(fields)
    spread = tip(weights)
    results = {}
    for first in range(0, groups, TOGETHER):
        now = steps[first : first + TOGETHER]
        parts = update(group, now, spread, deviation, mean)
        for s, part in zip(now, parts):
            results[s] = exchange(part.reshape(rows, columns), s, groups)
    placed = None
    for now in PLACED:
        positions = jnp.concatenate([order[s] for s in now]).reshape(-1, 1)
        positions = jnp.broadcast_to(positions, (positions.shape[0], LANES))
        placed = place_columns([results[s] for s in now], positions, placed, cells)
    return placed.reshape(own_members, quantities, cells)


def solution(mesh):
    return jax.shard_map(
        local_step,
        mesh=mesh,
        in_specs=(
            P("member", None, "grid"),
            P(None, None, "grid"),
            P("grid", None, "member"),
            P("grid", None, "member"),
            P(None, "grid"),
        ),
        out_specs=P("member", None, "grid"),
        check_vma=False,
    )
```
